8 devices in a mesh: fsdp: 8 (over z, y, x, core).
Axes of the slice: x: 2, y: 2, z: 1, core: 2. Of those that a mesh axis runs over, the one named last changes fastest.
Arguments:
- x_saved: bfloat16 [2, 16, 1536, 1536], P(None, 'fsdp')
- grad_out: bfloat16 [16, 1536, 1536], P('fsdp')
- x_next: bfloat16 [16, 1536, 1536], P('fsdp')
- w_up: bfloat16 [2, 1536, 6144], replicated
- w_down: bfloat16 [2, 6144, 1536], replicated
- gacc_up: float32 [2, 1536, 6144], P(None, 'fsdp')
- gacc_down: float32 [2, 6144, 1536], P(None, 'fsdp')
- master_up: float32 [2, 1536, 6144], P(None, 'fsdp')
- master_down: float32 [2, 6144, 1536], P(None, 'fsdp')
- mom1_up: float32 [2, 1536, 6144], P(None, 'fsdp')
- mom1_down: float32 [2, 6144, 1536], P(None, 'fsdp')
- mom2_up: float32 [2, 1536, 6144], P(None, 'fsdp')
- mom2_down: float32 [2, 6144, 1536], P(None, 'fsdp')
Outputs:
- output 1: bfloat16 [16, 1536, 1536], P('fsdp')
- output 2: float32 [2, 1536, 6144], P(None, 'fsdp')
- output 3: float32 [2, 6144, 1536], P(None, 'fsdp')
- output 4: float32 [2, 1536, 6144], P(None, 'fsdp')
- output 5: float32 [2, 6144, 1536], P(None, 'fsdp')
- output 6: float32 [2, 1536, 6144], P(None, 'fsdp')
- output 7: float32 [2, 6144, 1536], P(None, 'fsdp')
All inputs are finite; a program needn't handle non-finite values.
Results may differ from the reference program's by a relative error of at most 0.00830136.
Values are sent between devices in bfloat16 or wider.
A program may use at most 1 GiB of HBM per device.

```python
import math
import jax
import jax.numpy as jnp
from jax import lax

LAYERS = 2
ADAM_STEP = 3
MICRO_STEPS = 2
GROUP_DEVS = 8
GLOBAL_BATCH = 16
SEQ_LEN = 1536
D_MODEL = 1536
D_FF = 6144

DEV_BATCH = GLOBAL_BATCH // GROUP_DEVS
LEARN_RATE = 0.001
BETA_ONE = 0.9
BETA_TWO = 0.95
ADAM_EPS = 1e-8
WEIGHT_DECAY = 0.1
CLIP_NORM = 0.1 * math.sqrt(2 * LAYERS * D_MODEL * D_FF)


def setup_inputs(seed: int = 0) -> dict:
    key_list = jax.random.split(jax.random.key(seed), 13)
    up_scale = D_MODEL ** -0.5
    down_scale = D_FF ** -0.5
    tok_shape = (GLOBAL_BATCH, SEQ_LEN, D_MODEL)
    up_shape = (LAYERS, D_MODEL, D_FF)
    down_shape = (LAYERS, D_FF, D_MODEL)
    master_up = jax.random.normal(key_list[3], up_shape, jnp.float32) * up_scale
    master_down = jax.random.normal(key_list[4], down_shape, jnp.float32) * down_scale
    w_up = master_up + 0.3 * up_scale * jax.random.normal(key_list[5], up_shape, jnp.float32)
    w_down = master_down + 0.3 * down_scale * jax.random.normal(key_list[6], down_shape, jnp.float32)
    grad_scale = (GLOBAL_BATCH * SEQ_LEN) ** -0.5
    return {
        "x_saved": jax.random.normal(key_list[0], (LAYERS,) + tok_shape, jnp.float32).astype(jnp.bfloat16),
        "grad_out": (grad_scale * jax.random.normal(key_list[1], tok_shape, jnp.float32)).astype(jnp.bfloat16),
        "x_next": jax.random.normal(key_list[2], tok_shape, jnp.float32).astype(jnp.bfloat16),
        "w_up": w_up.astype(jnp.bfloat16),
        "w_down": w_down.astype(jnp.bfloat16),
        "gacc_up": 0.3 * jax.random.normal(key_list[7], up_shape, jnp.float32),
        "gacc_down": 0.6 * jax.random.normal(key_list[8], down_shape, jnp.float32),
        "master_up": master_up,
        "master_down": master_down,
        "mom1_up": 0.01 * jax.random.normal(key_list[9], up_shape, jnp.float32),
        "mom1_down": 0.01 * jax.random.normal(key_list[10], down_shape, jnp.float32),
        "mom2_up": 0.0004 * (0.5 + jax.random.uniform(key_list[11], up_shape, jnp.float32)),
        "mom2_down": 0.0004 * (0.5 + jax.random.uniform(key_list[12], down_shape, jnp.float32)),
    }


def gelu_fn(pre_act):
    return jax.nn.gelu(pre_act, approximate=True)


def seq_backward(w_up, w_down, x_layers, grad_seq):
    grads_up = []
    grads_down = []
    grad_cur = grad_seq
    for layer_idx in range(LAYERS - 1, -1, -1):
        x_in = x_layers[layer_idx]
        pre_act = jnp.dot(x_in, w_up[layer_idx], preferred_element_type=jnp.float32)
        hidden_act, gelu_vjp = jax.vjp(gelu_fn, pre_act)
        d_act = jnp.dot(grad_cur, w_down[layer_idx].T, preferred_element_type=jnp.float32)
        d_pre = gelu_vjp(d_act)[0].astype(jnp.bfloat16)
        grads_down.append(jnp.dot(hidden_act.astype(jnp.bfloat16).T, grad_cur, preferred_element_type=jnp.float32))
        grads_up.append(jnp.dot(x_in.T, d_pre, preferred_element_type=jnp.float32))
        if layer_idx > 0:
            grad_cur = (grad_cur.astype(jnp.float32) + jnp.dot(d_pre, w_up[layer_idx].T, preferred_element_type=jnp.float32)).astype(jnp.bfloat16)
    return jnp.stack(grads_up[::-1]), jnp.stack(grads_down[::-1])


def device_partials(w_up, w_down, x_dev, grad_dev):
    def scan_body(acc_in, seq_idx):
        up_grad, down_grad = seq_backward(w_up, w_down, x_dev[:, seq_idx], grad_dev[seq_idx])
        return (acc_in[0] + up_grad, acc_in[1] + down_grad), None
    start_acc = (jnp.zeros((LAYERS, D_MODEL, D_FF), jnp.float32), jnp.zeros((LAYERS, D_FF, D_MODEL), jnp.float32))
    acc_pair, _ = lax.scan(scan_body, start_acc, jnp.arange(DEV_BATCH))
    return acc_pair[0].astype(jnp.bfloat16), acc_pair[1].astype(jnp.bfloat16)


def adamw_update(master_old, mom_one, mom_two, grad_clip):
    mom_one_new = BETA_ONE * mom_one + (1.0 - BETA_ONE) * grad_clip
    mom_two_new = BETA_TWO * mom_two + (1.0 - BETA_TWO) * grad_clip * grad_clip
    first_hat = mom_one_new / (1.0 - BETA_ONE ** ADAM_STEP)
    second_hat = mom_two_new / (1.0 - BETA_TWO ** ADAM_STEP)
    master_new = master_old - LEARN_RATE * (first_hat / (jnp.sqrt(second_hat) + ADAM_EPS) + WEIGHT_DECAY * master_old)
    return master_new, mom_one_new, mom_two_new


def seq_forward(w_up_new, w_down_new, x_seq):
    hidden_state = x_seq
    for layer_idx in range(LAYERS):
        pre_act = jnp.dot(hidden_state, w_up_new[layer_idx], preferred_element_type=jnp.float32)
        hidden_act = gelu_fn(pre_act).astype(jnp.bfloat16)
        hidden_state = (hidden_state.astype(jnp.float32) + jnp.dot(hidden_act, w_down_new[layer_idx], preferred_element_type=jnp.float32)).astype(jnp.bfloat16)
    return hidden_state


def reference(x_saved, grad_out, x_next, w_up, w_down, gacc_up, gacc_down, master_up, master_down, mom1_up, mom1_down, mom2_up, mom2_down):
    x_groups = x_saved.reshape(LAYERS, GROUP_DEVS, DEV_BATCH, SEQ_LEN, D_MODEL)
    grad_groups = grad_out.reshape(GROUP_DEVS, DEV_BATCH, SEQ_LEN, D_MODEL)

    def dev_body(acc_in, dev_idx):
        part_up, part_down = device_partials(w_up, w_down, x_groups[:, dev_idx], grad_groups[dev_idx])
        return (acc_in[0] + part_up.astype(jnp.float32), acc_in[1] + part_down.astype(jnp.float32)), None

    start_acc = (jnp.zeros((LAYERS, D_MODEL, D_FF), jnp.float32), jnp.zeros((LAYERS, D_FF, D_MODEL), jnp.float32))
    acc_pair, _ = lax.scan(dev_body, start_acc, jnp.arange(GROUP_DEVS))
    grad_up = (gacc_up + acc_pair[0]) / MICRO_STEPS
    grad_down = (gacc_down + acc_pair[1]) / MICRO_STEPS
    total_norm = jnp.sqrt(jnp.sum(grad_up * grad_up) + jnp.sum(grad_down * grad_down))
    clip_factor = jnp.minimum(1.0, CLIP_NORM / total_norm)
    new_up = adamw_update(master_up, mom1_up, mom2_up, grad_up * clip_factor)
    new_down = adamw_update(master_down, mom1_down, mom2_down, grad_down * clip_factor)
    w_up_new = new_up[0].astype(jnp.bfloat16)
    w_down_new = new_down[0].astype(jnp.bfloat16)
    x_out = lax.map(lambda x_seq: seq_forward(w_up_new, w_down_new, x_seq), x_next)
    return (x_out, new_up[0], new_down[0], new_up[1], new_down[1], new_up[2], new_down[2])
```

```python
import functools
import math
import jax
import jax.numpy as jnp
from jax import lax
from jax.experimental import pallas as pl
from jax.experimental.pallas import tpu as pltpu
from jax.sharding import PartitionSpec as P

LEARN_RATE = 0.001
BETA_ONE = 0.9
BETA_TWO = 0.95
ADAM_EPS = 1e-8
WEIGHT_DECAY = 0.1
ADAM_STEP = 3
MICRO_STEPS = 2

GELU_LIN = 0.7978845608028654
GELU_CUB = GELU_LIN * 0.044715
PAIR_SWAP = [(0, 1), (1, 0), (2, 3), (3, 2), (4, 5), (5, 4), (6, 7), (7, 6)]
SAME_CORE = [[0, 2, 4, 6], [1, 3, 5, 7]]
LANES = 256
TOK = 1024
FF = 768
VMEM_BYTES = 56 * 2**20
NN = (((1,), (0,)), ((), ()))
NT = (((1,), (1,)), ((), ()))
TN = (((0,), (0,)), ((), ()))


def fdot(left, right, dims):
    return lax.dot_general(left, right, dims, preferred_element_type=jnp.float32)


def params():
    return pltpu.CompilerParams(vmem_limit_bytes=VMEM_BYTES)


def cost(flops, moved, trans=0):
    return pl.CostEstimate(flops=int(flops), bytes_accessed=int(moved), transcendentals=int(trans))


def act_dpre_kernel(core_ref, x_ref, g_ref, up_ref, down_ref, act_ref, dpre_ref):
    for start in range(0, up_ref.shape[1], LANES):
        cols = slice(start, start + LANES)
        pre = fdot(x_ref[...], up_ref[:, cols], NN)
        d_act = fdot(g_ref[...], down_ref[cols, :], NT)
        square = pre * pre
        tanh_val = jnp.tanh(pre * (GELU_LIN + GELU_CUB * square))
        cdf = 0.5 + 0.5 * tanh_val
        slope = cdf + (0.5 * pre) * (1.0 - tanh_val * tanh_val) * (GELU_LIN + 3.0 * GELU_CUB * square)
        act_ref[:, cols] = (pre * cdf).astype(jnp.bfloat16)
        dpre_ref[:, cols] = (d_act * slope).astype(jnp.bfloat16)


def act_and_dpre(core, x_all, grad, w_up, w_down, layer):
    tokens, width = grad.shape
    ff = w_up.shape[2]
    tiles = tokens // TOK
    spec = pltpu.PrefetchScalarGridSpec(
        num_scalar_prefetch=1,
        grid=(tiles, ff // FF // 2),
        in_specs=[
            pl.BlockSpec((TOK, width), lambda i, j, c: (layer * tiles + i, 0)),
            pl.BlockSpec((TOK, width), lambda i, j, c: (i, 0)),
            pl.BlockSpec((None, width, FF), lambda i, j, c: (layer, 0, 2 * j + c[0])),
            pl.BlockSpec((None, FF, width), lambda i, j, c: (layer, 2 * j + c[0], 0)),
        ],
        out_specs=[pl.BlockSpec((TOK, FF), lambda i, j, c: (i, j))] * 2,
    )
    return pl.pallas_call(
        act_dpre_kernel,
        out_shape=[jax.ShapeDtypeStruct((tokens, ff // 2), jnp.bfloat16)] * 2,
        grid_spec=spec,
        compiler_params=params(),
        cost_estimate=cost(2 * tokens * width * ff, 4 * tokens * width + 2 * tokens * ff + 6 * width * ff, tokens * ff // 2),
        name="act_dpre",
    )(core, x_all, grad, w_up, w_down)


def back_kernel(parts, final, core_ref, dpre_ref, *refs):
    w_refs, refs = refs[:parts], refs[parts:]
    out_ref = refs[-1]
    for start in range(0, out_ref.shape[1], LANES):
        cols = slice(start, start + LANES)
        total = fdot(dpre_ref[:, 0:FF], w_refs[0][cols, :], NT)
        for q in range(1, parts):
            total += fdot(dpre_ref[:, q * FF:(q + 1) * FF], w_refs[q][cols, :], NT)
        if final:
            total = refs[0][:, cols].astype(jnp.float32) + (total + refs[1][:, cols])
        out_ref[:, cols] = total.astype(out_ref.dtype)


def grad_back(core, dpre, w_up, layer, extra=()):
    tokens, half = dpre.shape
    width = w_up.shape[1]
    parts = half // FF
    col_tile = width // 2
    tile = pl.BlockSpec((TOK, col_tile), lambda i, j, c: (i, j))
    w_specs = [pl.BlockSpec((None, col_tile, FF), functools.partial(lambda q, i, j, c: (layer, j, 2 * q + c[0]), q)) for q in range(parts)]
    spec = pltpu.PrefetchScalarGridSpec(
        num_scalar_prefetch=1,
        grid=(tokens // TOK, width // col_tile),
        in_specs=[pl.BlockSpec((TOK, half), lambda i, j, c: (i, 0))] + w_specs + [tile] * len(extra),
        out_specs=tile,
    )
    return pl.pallas_call(
        functools.partial(back_kernel, parts, bool(extra)),
        out_shape=jax.ShapeDtypeStruct((tokens, width), jnp.bfloat16 if extra else jnp.float32),
        grid_spec=spec,
        compiler_params=params(),
        cost_estimate=cost(2 * tokens * half * width, 2 * tokens * half + 4 * width * half + 6 * tokens * width),
        name="grad_back",
    )(core, dpre, *([w_up] * parts), *extra)


def token_dot_kernel(left_own, right_own, left_peer, right_peer, out_ref, total):
    k = pl.program_id(2)

    @pl.when(k == 0)
    def _():
        total[...] = fdot(left_own[...], right_own[...], TN)

    @pl.when(k == 1)
    def _():
        total[...] += fdot(left_own[...], right_own[...], TN)

    @pl.when(k == 2)
    def _():
        total[...] += fdot(left_peer[...], right_peer[...], TN)

    @pl.when(k == 3)
    def _():
        out_ref[...] = (total[...] + fdot(left_peer[...], right_peer[...], TN)).astype(jnp.bfloat16)


def token_dot(left_own, right_own, left_peer, right_peer, tokens, tile, left_row=0):
    rows, cols = left_own.shape[1], right_own.shape[1]
    depth = tokens // 2
    row_tile, col_tile = tile

    def block(width, axis, first, row):
        def index(i, j, k):
            step = jnp.minimum(k, 1) if first else jnp.maximum(k - 2, 0)
            return (row + step, (i, j)[axis])
        return pl.BlockSpec((depth, width), index)

    return pl.pallas_call(
        token_dot_kernel,
        out_shape=jax.ShapeDtypeStruct((rows, cols), jnp.bfloat16),
        grid=(rows // row_tile, cols // col_tile, 4),
        in_specs=[block(row_tile, 0, True, left_row), block(col_tile, 1, True, 0), block(row_tile, 0, False, left_row), block(col_tile, 1, False, 0)],
        out_specs=pl.BlockSpec((row_tile, col_tile), lambda i, j, k: (i, j)),
        scratch_shapes=[pltpu.VMEM((row_tile, col_tile), jnp.float32)],
        compiler_params=params(),
        cost_estimate=cost(4 * tokens * rows * cols, 4 * tokens * (rows + cols) + 2 * rows * cols),
        name="token_dot",
    )(left_own, right_own, left_peer, right_peer)


def sum_kernel(recv_ref, acc_ref, grad_ref, sq_ref):
    total = recv_ref[0].astype(jnp.float32)
    for src in range(1, recv_ref.shape[0]):
        total += recv_ref[src].astype(jnp.float32)
    grad = (acc_ref[...] + total) * (1.0 / MICRO_STEPS)
    grad_ref[...] = grad
    square = jnp.sum((grad * grad).reshape(-1, 8, grad.shape[1]), axis=0)
    first = pl.program_id(0) == 0
    for axis in range(1, 2):
        first = jnp.logical_and(first, pl.program_id(axis) == 0)

    @pl.when(first)
    def _():
        sq_ref[...] = square

    @pl.when(jnp.logical_not(first))
    def _():
        sq_ref[...] += square


def summed(recv, gacc, layer, grid, recv_block, recv_index, tile, index):
    rows, cols = gacc.shape[1:]
    return pl.pallas_call(
        sum_kernel,
        out_shape=[jax.ShapeDtypeStruct((rows, cols), jnp.float32), jax.ShapeDtypeStruct((8, tile[1]), jnp.float32)],
        grid=grid,
        in_specs=[pl.BlockSpec(recv_block, recv_index), pl.BlockSpec((None,) + tile, lambda a, b: (layer,) + index(a, b))],
        out_specs=[pl.BlockSpec(tile, index), pl.BlockSpec((8, tile[1]), lambda a, b: (0, 0))],
        compiler_params=params(),
        cost_estimate=cost(8 * rows * cols, 16 * rows * cols),
        name="grad_sum",
    )(recv, gacc)


def norm_kernel(n_dev, clip_norm, part_ref, clip_ref, slots, send_sem, recv_sem):
    me = lax.axis_index("fsdp")
    barrier = pltpu.get_barrier_semaphore()
    for step in range(1, n_dev):
        pl.semaphore_signal(barrier, inc=1, device_id=(lax.rem(me + step, n_dev),), device_id_type=pl.DeviceIdType.MESH)
    pl.semaphore_wait(barrier, n_dev - 1)

    def copy_to(step):
        return pltpu.make_async_remote_copy(
            src_ref=part_ref,
            dst_ref=slots.at[step],
            send_sem=send_sem.at[step],
            recv_sem=recv_sem.at[step],
            device_id=(lax.rem(me + step, n_dev),),
            device_id_type=pl.DeviceIdType.MESH,
        )

    for step in range(1, n_dev):
        copy_to(step).start()
    for step in range(1, n_dev):
        copy_to(step).wait()
    total = part_ref[...]
    for step in range(1, n_dev):
        total = total + slots[step]
    norm = jnp.sqrt(jnp.sum(total, keepdims=True))
    clip_ref[...] = jnp.broadcast_to(jnp.minimum(1.0, clip_norm / norm), clip_ref.shape)


def clip_factor(part, n_dev, clip_norm):
    return pl.pallas_call(
        functools.partial(norm_kernel, n_dev, clip_norm),
        out_shape=jax.ShapeDtypeStruct((8, 128), jnp.float32),
        in_specs=[pl.BlockSpec(memory_space=pltpu.VMEM)],
        out_specs=pl.BlockSpec(memory_space=pltpu.VMEM),
        scratch_shapes=[pltpu.VMEM((n_dev, 8, 128), jnp.float32), pltpu.SemaphoreType.DMA((n_dev,)), pltpu.SemaphoreType.DMA((n_dev,))],
        compiler_params=pltpu.CompilerParams(collective_id=0, has_side_effects=True),
        name="clip_norm",
    )(part)


def adamw_kernel(aliased, clip_ref, grad_ref, master_ref, one_ref, two_ref, *refs):
    new_master_ref, new_one_ref, new_two_ref, weight_ref = refs[aliased:]
    grad = grad_ref[...] * clip_ref[0:1, 0:1]
    master = master_ref[...]
    one = BETA_ONE * one_ref[...] + (1.0 - BETA_ONE) * grad
    two = BETA_TWO * two_ref[...] + (1.0 - BETA_TWO) * grad * grad
    first_hat = one / (1.0 - BETA_ONE ** ADAM_STEP)
    second_hat = two / (1.0 - BETA_TWO ** ADAM_STEP)
    master = master - LEARN_RATE * (first_hat / (jnp.sqrt(second_hat) + ADAM_EPS) + WEIGHT_DECAY * master)
    new_one_ref[...] = one
    new_two_ref[...] = two
    new_master_ref[...] = master
    weight_ref[...] = master.astype(jnp.bfloat16)


def adamw(clip, grad, master, mom_one, mom_two, layer, tile, earlier=()):
    rows, cols = grad.shape
    index = lambda a, b: (a, b)
    whole = pl.BlockSpec((None,) + tile, lambda a, b: (layer, a, b))
    part = pl.BlockSpec(tile, index)
    full = jax.ShapeDtypeStruct(master.shape, jnp.float32)
    return pl.pallas_call(
        functools.partial(adamw_kernel, len(earlier)),
        out_shape=[full] * 3 + [jax.ShapeDtypeStruct((rows, cols), jnp.bfloat16)],
        grid=(rows // tile[0], cols // tile[1]),
        in_specs=[pl.BlockSpec((8, 128), lambda a, b: (0, 0)), part, whole, whole, whole] + [pl.BlockSpec(memory_space=pl.ANY)] * len(earlier),
        out_specs=[whole] * 3 + [part],
        input_output_aliases={5 + i: i for i in range(len(earlier))},
        compiler_params=params(),
        cost_estimate=cost(20 * rows * cols, 30 * rows * cols, 2 * rows * cols),
        name="adamw",
    )(clip, grad, master, mom_one, mom_two, *earlier)


def up_kernel(x_ref, w_ref, act_ref):
    for start in range(0, w_ref.shape[1], LANES):
        cols = slice(start, start + LANES)
        pre = fdot(x_ref[...], w_ref[:, cols], NN)
        cdf = 0.5 + 0.5 * jnp.tanh(pre * (GELU_LIN + GELU_CUB * (pre * pre)))
        act_ref[:, cols] = (pre * cdf).astype(jnp.bfloat16)


def forward_up(hidden, weight):
    tokens, width = hidden.shape
    ff = weight.shape[1]
    return pl.pallas_call(
        up_kernel,
        out_shape=jax.ShapeDtypeStruct((tokens, ff), jnp.bfloat16),
        grid=(tokens // TOK, ff // FF),
        in_specs=[pl.BlockSpec((TOK, width), lambda i, j: (i, 0)), pl.BlockSpec((width, FF), lambda i, j: (0, j))],
        out_specs=pl.BlockSpec((TOK, FF), lambda i, j: (i, j)),
        compiler_params=params(),
        cost_estimate=cost(2 * tokens * width * ff, 2 * tokens * width + 2 * tokens * ff + 2 * width * ff, tokens * ff),
        name="forward_up",
    )(hidden, weight)


def down_kernel(act_ref, w_ref, hidden_ref, out_ref, total):
    k = pl.program_id(2)
    last = pl.num_programs(2) - 1

    @pl.when(k == 0)
    def _():
        total[...] = fdot(act_ref[...], w_ref[...], NN)

    @pl.when(jnp.logical_and(k > 0, k < last))
    def _():
        total[...] += fdot(act_ref[...], w_ref[...], NN)

    @pl.when(k == last)
    def _():
        out_ref[...] = (hidden_ref[...].astype(jnp.float32) + (total[...] + fdot(act_ref[...], w_ref[...], NN))).astype(jnp.bfloat16)


def forward_down(act, weight, hidden):
    tokens, ff = act.shape
    width = weight.shape[1]
    col_tile, depth = width // 2, 2 * FF
    tile = pl.BlockSpec((TOK, col_tile), lambda i, j, k: (i, j))
    return pl.pallas_call(
        down_kernel,
        out_shape=jax.ShapeDtypeStruct((tokens, width), jnp.bfloat16),
        grid=(tokens // TOK, width // col_tile, ff // depth),
        in_specs=[pl.BlockSpec((TOK, depth), lambda i, j, k: (i, k)), pl.BlockSpec((depth, col_tile), lambda i, j, k: (k, j)), tile],
        out_specs=tile,
        scratch_shapes=[pltpu.VMEM((TOK, col_tile), jnp.float32)],
        compiler_params=params(),
        cost_estimate=cost(2 * tokens * width * ff, 2 * tokens * ff + 4 * tokens * width + 2 * width * ff),
        name="forward_down",
    )(act, weight, hidden)


def pair_swap(value):
    return lax.ppermute(value, "fsdp", PAIR_SWAP)


def after(value, *first):
    return lax.optimization_barrier((value,) + first)[0]


def gradient_rows(x_saved, grad_out, w_up, w_down, gacc_up, gacc_down):
    layers, width, ff = w_up.shape
    core = lax.rem(lax.axis_index("fsdp"), 2).reshape(1)
    x_own = x_saved.reshape(-1, width)
    grad_own = grad_out.reshape(-1, width)
    tokens = grad_own.shape[0]
    x_peer, grad_peer = pair_swap(x_own), pair_swap(grad_own)
    rows_up, rows_down = [None] * layers, [None] * layers
    recv_down = None
    for layer in range(layers - 1, -1, -1):
        act_own, dpre_own = act_and_dpre(core, x_own, grad_own, w_up, w_down, layer)
        peer_core = after(core, act_own) if recv_down is None else after(core, act_own, recv_down)
        act_peer, dpre_peer = act_and_dpre(peer_core, x_peer, grad_peer, w_up, w_down, layer)
        old_grads = (grad_own, grad_peer)
        if layer > 0:
            from_peer = pair_swap(grad_back(core, dpre_peer, w_up, layer))
            grad_own = grad_back(core, dpre_own, w_up, layer, (grad_own, from_peer))
            grad_peer = pair_swap(grad_own)
        part_down = token_dot(act_own, old_grads[0], act_peer, old_grads[1], tokens, (TOK, FF))
        recv_down = lax.all_to_all(part_down, "fsdp", 0, 0, tiled=True, axis_index_groups=SAME_CORE)
        part_up = token_dot(x_own, dpre_own, x_peer, dpre_peer, tokens, (FF, TOK), layer * 2)
        recv_up = lax.all_to_all(part_up, "fsdp", 0, 0, tiled=True)
        rows_down[layer] = summed(recv_down.reshape(4, -1, width), gacc_down, layer, (4, 1), (4, 192, width), lambda a, b: (0, a, 0), (192, width), lambda a, b: (a, 0))
        rows_up[layer] = summed(recv_up.reshape(4, 2, -1, ff // 2), gacc_up, layer, (4, 2), (4, None, 192, FF), lambda a, b: (0, b, 0, a), (192, FF), lambda a, b: (0, 2 * a + b))
    return rows_up, rows_down


def solution(mesh):
    n_dev = mesh.shape["fsdp"]
    rows_spec = P(None, "fsdp")

    def local_step(x_saved, grad_out, x_next, w_up, w_down, gacc_up, gacc_down, master_up, master_down, mom1_up, mom1_down, mom2_up, mom2_down):
        layers, width, ff = w_up.shape
        clip_norm = 0.1 * math.sqrt(2 * layers * width * ff)
        rows_up, rows_down = gradient_rows(x_saved, grad_out, w_up, w_down, gacc_up, gacc_down)
        part = sum(jnp.sum(sq.reshape(8, -1, 128), axis=1) for _, sq in rows_up + rows_down)
        clip = clip_factor(part, n_dev, clip_norm)
        new_up, new_down = (), ()
        up_shards, down_shards = [], []
        for layer in range(layers):
            *new_up, shard = adamw(clip, rows_up[layer][0], master_up, mom1_up, mom2_up, layer, (192, FF), new_up)
            up_shards.append(shard)
            *new_down, shard = adamw(clip, rows_down[layer][0], master_down, mom1_down, mom2_down, layer, (96, width), new_down)
            down_shards.append(shard)
        hidden = x_next.reshape(-1, width)
        for layer in range(layers):
            act = forward_up(hidden, lax.all_gather(up_shards[layer], "fsdp", axis=0, tiled=True))
            hidden = forward_down(act, lax.all_gather(down_shards[layer], "fsdp", axis=0, tiled=True), hidden)
        return (hidden.reshape(x_next.shape), new_up[0], new_down[0], new_up[1], new_down[1], new_up[2], new_down[2])

    return jax.shard_map(local_step, mesh=mesh, in_specs=(rows_spec, P("fsdp"), P("fsdp"), P(), P(), rows_spec, rows_spec, rows_spec, rows_spec, rows_spec, rows_spec, rows_spec, rows_spec), out_specs=(P("fsdp"), rows_spec, rows_spec, rows_spec, rows_spec, rows_spec, rows_spec), check_vma=False)
```

```python
import functools
import math
import jax
import jax.numpy as jnp
from jax import lax
from jax.experimental import pallas as pl
from jax.experimental.pallas import tpu as pltpu
from jax.sharding import PartitionSpec as P

LEARN_RATE = 0.001
BETA_ONE = 0.9
BETA_TWO = 0.95
ADAM_EPS = 1e-8
WEIGHT_DECAY = 0.1
ADAM_STEP = 3
MICRO_STEPS = 2

GELU_LIN = 0.7978845608028654
GELU_CUB = GELU_LIN * 0.044715
PAIR_SWAP = [(0, 1), (1, 0), (2, 3), (3, 2), (4, 5), (5, 4), (6, 7), (7, 6)]
SAME_CORE = [[0, 2, 4, 6], [1, 3, 5, 7]]
LANES = 256
TOK = 1024
SUB = 256
FF = 768
DEPTH = 768
WIDE = 1536
VMEM_BYTES = 56 * 2**20
NN = (((1,), (0,)), ((), ()))
NT = (((1,), (1,)), ((), ()))
TN = (((0,), (0,)), ((), ()))


def fdot(left, right, dims):
    return lax.dot_general(left, right, dims, preferred_element_type=jnp.float32)


def params():
    return pltpu.CompilerParams(vmem_limit_bytes=VMEM_BYTES)


def cost(flops, moved, trans=0):
    return pl.CostEstimate(flops=int(flops), bytes_accessed=int(moved), transcendentals=int(trans))


def act_dpre_kernel(core_ref, x_ref, g_ref, up_ref, down_ref, act_ref, dpre_ref):
    for start in range(0, up_ref.shape[1], LANES):
        cols = slice(start, start + LANES)
        for top in range(0, x_ref.shape[0], SUB):
            rows = slice(top, top + SUB)
            pre = fdot(x_ref[rows, :], up_ref[:, cols], NN)
            d_act = fdot(g_ref[rows, :], down_ref[cols, :], NT)
            square = pre * pre
            cdf = 0.5 + 0.5 * jnp.tanh(pre * (GELU_LIN + GELU_CUB * square))
            act = pre * cdf
            slope = cdf + (act * (1.0 - cdf)) * (2.0 * GELU_LIN + 6.0 * GELU_CUB * square)
            act_ref[rows, cols] = act.astype(jnp.bfloat16)
            dpre_ref[rows, cols] = (d_act * slope).astype(jnp.bfloat16)


def act_and_dpre(core, x_all, grad, w_up, w_down, layer):
    tokens, width = grad.shape
    ff = w_up.shape[2]
    tiles = tokens // TOK
    spec = pltpu.PrefetchScalarGridSpec(
        num_scalar_prefetch=1,
        grid=(tiles, ff // FF // 2),
        in_specs=[
            pl.BlockSpec((TOK, width), lambda i, j, c: (layer * tiles + i, 0)),
            pl.BlockSpec((TOK, width), lambda i, j, c: (i, 0)),
            pl.BlockSpec((None, width, FF), lambda i, j, c: (layer, 0, 2 * j + c[0])),
            pl.BlockSpec((None, FF, width), lambda i, j, c: (layer, 2 * j + c[0], 0)),
        ],
        out_specs=[pl.BlockSpec((TOK, FF), lambda i, j, c: (i, j))] * 2,
    )
    return pl.pallas_call(
        act_dpre_kernel,
        out_shape=[jax.ShapeDtypeStruct((tokens, ff // 2), jnp.bfloat16)] * 2,
        grid_spec=spec,
        compiler_params=params(),
        cost_estimate=cost(2 * tokens * width * ff, 4 * tokens * width + 2 * tokens * ff + 6 * width * ff, tokens * ff // 2),
        name="act_dpre",
    )(core, x_all, grad, w_up, w_down)


def back_kernel(parts, final, core_ref, dpre_ref, *refs):
    w_refs, refs = refs[:parts], refs[parts:]
    out_ref = refs[-1]
    for start in range(0, out_ref.shape[1], LANES):
        cols = slice(start, start + LANES)
        total = fdot(dpre_ref[:, 0:FF], w_refs[0][cols, :], NT)
        for q in range(1, parts):
            total += fdot(dpre_ref[:, q * FF:(q + 1) * FF], w_refs[q][cols, :], NT)
        if final:
            total = refs[0][:, cols].astype(jnp.float32) + (total + refs[1][:, cols])
        out_ref[:, cols] = total.astype(out_ref.dtype)


def grad_back(core, dpre, w_up, layer, extra=()):
    tokens, half = dpre.shape
    width = w_up.shape[1]
    parts = half // FF
    col_tile = width // 2
    tile = pl.BlockSpec((TOK, col_tile), lambda i, j, c: (i, j))
    w_specs = [pl.BlockSpec((None, col_tile, FF), functools.partial(lambda q, i, j, c: (layer, j, 2 * q + c[0]), q)) for q in range(parts)]
    spec = pltpu.PrefetchScalarGridSpec(
        num_scalar_prefetch=1,
        grid=(tokens // TOK, width // col_tile),
        in_specs=[pl.BlockSpec((TOK, half), lambda i, j, c: (i, 0))] + w_specs + [tile] * len(extra),
        out_specs=tile,
    )
    return pl.pallas_call(
        functools.partial(back_kernel, parts, bool(extra)),
        out_shape=jax.ShapeDtypeStruct((tokens, width), jnp.bfloat16 if extra else jnp.float32),
        grid_spec=spec,
        compiler_params=params(),
        cost_estimate=cost(2 * tokens * half * width, 2 * tokens * half + 4 * width * half + 6 * tokens * width),
        name="grad_back",
    )(core, dpre, *([w_up] * parts), *extra)


def token_dot_kernel(order_ref, left_own, right_own, left_peer, right_peer, out_ref, total):
    k = pl.program_id(2)
    last = pl.num_programs(2) - 1
    odd = lax.rem(k, 2)

    @pl.when(k == 0)
    def _():
        total[...] = fdot(left_own[...], right_own[...], TN)

    @pl.when(jnp.logical_and(k > 0, odd == 0))
    def _():
        total[...] += fdot(left_own[...], right_own[...], TN)

    @pl.when(jnp.logical_and(k < last, odd == 1))
    def _():
        total[...] += fdot(left_peer[...], right_peer[...], TN)

    @pl.when(k == last)
    def _():
        out_ref[...] = (total[...] + fdot(left_peer[...], right_peer[...], TN)).astype(jnp.bfloat16)


def token_dot(order, left_own, right_own, left_peer, right_peer, tokens, tile, left_row=0, cols=None, right_col=0):
    rows = left_own.shape[1]
    cols = cols or right_own.shape[1]
    row_tile, col_tile = tile
    steps = tokens // DEPTH

    def left(own):
        return pl.BlockSpec((DEPTH, row_tile), lambda i, j, k, c: (left_row * steps + (k // 2 if own else jnp.maximum(k - 1, 0) // 2), i))

    def right(own):
        return pl.BlockSpec((DEPTH, col_tile), lambda i, j, k, c: (k // 2 if own else jnp.maximum(k - 1, 0) // 2, right_col + j))

    spec = pltpu.PrefetchScalarGridSpec(
        num_scalar_prefetch=1,
        grid=(rows // row_tile, cols // col_tile, 2 * steps),
        in_specs=[left(True), right(True), left(False), right(False)],
        out_specs=pl.BlockSpec((row_tile, col_tile), lambda i, j, k, c: (i, j)),
        scratch_shapes=[pltpu.VMEM((row_tile, col_tile), jnp.float32)],
    )
    return pl.pallas_call(
        token_dot_kernel,
        out_shape=jax.ShapeDtypeStruct((rows, cols), jnp.bfloat16),
        grid_spec=spec,
        compiler_params=params(),
        cost_estimate=cost(4 * tokens * rows * cols, 4 * tokens * (rows + cols) + 2 * rows * cols),
        name="token_dot",
    )(order, left_own, right_own, left_peer, right_peer)


def sum_kernel(recv_ref, acc_ref, *refs):
    grad_ref, sq_ref = refs[-2:]
    total = recv_ref[0].astype(jnp.float32)
    for src in range(1, recv_ref.shape[0]):
        total += recv_ref[src].astype(jnp.float32)
    grad = (acc_ref[...] + total) * (1.0 / MICRO_STEPS)
    grad_ref[...] = grad
    square = jnp.sum((grad * grad).reshape(-1, 8, grad.shape[1]), axis=0)
    first = pl.program_id(0) == 0
    for axis in range(1, 2):
        first = jnp.logical_and(first, pl.program_id(axis) == 0)

    @pl.when(first)
    def _():
        sq_ref[...] = square

    @pl.when(jnp.logical_not(first))
    def _():
        sq_ref[...] += square


def summed(recv, gacc, layer, grid, recv_block, recv_index, tile, index, earlier=()):
    rows, cols = gacc.shape[1:]
    moved = recv.size * 2 + recv.size * 2
    return pl.pallas_call(
        sum_kernel,
        out_shape=[jax.ShapeDtypeStruct((rows, cols), jnp.float32), jax.ShapeDtypeStruct((8, tile[1]), jnp.float32)],
        grid=grid,
        in_specs=[pl.BlockSpec(recv_block, recv_index), pl.BlockSpec((None,) + tile, lambda a, b: (layer,) + index(a, b))] + [pl.BlockSpec(memory_space=pl.ANY)] * len(earlier),
        out_specs=[pl.BlockSpec(tile, index), pl.BlockSpec((8, tile[1]), lambda a, b: (0, 0))],
        input_output_aliases={2 + i: i for i in range(len(earlier))},
        compiler_params=params(),
        cost_estimate=cost(2 * recv.size, moved),
        name="grad_sum",
    )(recv, gacc, *earlier)


def summed_down(recv, gacc, layer, first_col, earlier=()):
    width = recv.shape[1]
    tile = (192, 512)
    skip = first_col // tile[1]
    return summed(recv.reshape(4, -1, width), gacc, layer, (4, width // tile[1]), (4,) + tile, lambda a, b: (0, a, b), tile, lambda a, b: (a, skip + b), earlier)


def summed_up(recv, gacc, layer):
    tile = (192, FF)
    return summed(recv.reshape(4, 2, -1, recv.shape[1]), gacc, layer, (4, 2), (4, None) + tile, lambda a, b: (0, b, 0, a), tile, lambda a, b: (0, 2 * a + b))


def norm_kernel(n_dev, clip_norm, part_ref, clip_ref, slots, send_sem, recv_sem):
    me = lax.axis_index("fsdp")
    barrier = pltpu.get_barrier_semaphore()
    for step in range(1, n_dev):
        pl.semaphore_signal(barrier, inc=1, device_id=(lax.rem(me + step, n_dev),), device_id_type=pl.DeviceIdType.MESH)
    pl.semaphore_wait(barrier, n_dev - 1)

    def copy_to(step):
        return pltpu.make_async_remote_copy(
            src_ref=part_ref,
            dst_ref=slots.at[step],
            send_sem=send_sem.at[step],
            recv_sem=recv_sem.at[step],
            device_id=(lax.rem(me + step, n_dev),),
            device_id_type=pl.DeviceIdType.MESH,
        )

    for step in range(1, n_dev):
        copy_to(step).start()
    for step in range(1, n_dev):
        copy_to(step).wait()
    total = part_ref[...]
    for step in range(1, n_dev):
        total = total + slots[step]
    norm = jnp.sqrt(jnp.sum(total, keepdims=True))
    clip_ref[...] = jnp.broadcast_to(jnp.minimum(1.0, clip_norm / norm), clip_ref.shape)


def clip_factor(part, n_dev, clip_norm):
    return pl.pallas_call(
        functools.partial(norm_kernel, n_dev, clip_norm),
        out_shape=jax.ShapeDtypeStruct((8, 128), jnp.float32),
        in_specs=[pl.BlockSpec(memory_space=pltpu.VMEM)],
        out_specs=pl.BlockSpec(memory_space=pltpu.VMEM),
        scratch_shapes=[pltpu.VMEM((n_dev, 8, 128), jnp.float32), pltpu.SemaphoreType.DMA((n_dev,)), pltpu.SemaphoreType.DMA((n_dev,))],
        compiler_params=pltpu.CompilerParams(collective_id=0, has_side_effects=True),
        name="clip_norm",
    )(part)


def adamw_kernel(aliased, clip_ref, grad_ref, master_ref, one_ref, two_ref, *refs):
    new_master_ref, new_one_ref, new_two_ref, weight_ref = refs[aliased:]
    grad = grad_ref[...] * clip_ref[0:1, 0:1]
    master = master_ref[...]
    one = BETA_ONE * one_ref[...] + (1.0 - BETA_ONE) * grad
    two = BETA_TWO * two_ref[...] + (1.0 - BETA_TWO) * grad * grad
    first_hat = one / (1.0 - BETA_ONE ** ADAM_STEP)
    second_hat = two / (1.0 - BETA_TWO ** ADAM_STEP)
    master = master - LEARN_RATE * (first_hat / (jnp.sqrt(second_hat) + ADAM_EPS) + WEIGHT_DECAY * master)
    new_one_ref[...] = one
    new_two_ref[...] = two
    new_master_ref[...] = master
    weight_ref[...] = master.astype(jnp.bfloat16)


def adamw(clip, grad, master, mom_one, mom_two, layer, tile, earlier=()):
    rows, cols = grad.shape
    index = lambda a, b: (a, b)
    whole = pl.BlockSpec((None,) + tile, lambda a, b: (layer, a, b))
    part = pl.BlockSpec(tile, index)
    full = jax.ShapeDtypeStruct(master.shape, jnp.float32)
    return pl.pallas_call(
        functools.partial(adamw_kernel, len(earlier)),
        out_shape=[full] * 3 + [jax.ShapeDtypeStruct((rows, cols), jnp.bfloat16)],
        grid=(rows // tile[0], cols // tile[1]),
        in_specs=[pl.BlockSpec((8, 128), lambda a, b: (0, 0)), part, whole, whole, whole] + [pl.BlockSpec(memory_space=pl.ANY)] * len(earlier),
        out_specs=[whole] * 3 + [part],
        input_output_aliases={5 + i: i for i in range(len(earlier))},
        compiler_params=params(),
        cost_estimate=cost(20 * rows * cols, 30 * rows * cols, 2 * rows * cols),
        name="adamw",
    )(clip, grad, master, mom_one, mom_two, *earlier)


def up_kernel(x_ref, w_ref, act_ref):
    for start in range(0, w_ref.shape[1], LANES):
        cols = slice(start, start + LANES)
        for top in range(0, x_ref.shape[0], SUB):
            rows = slice(top, top + SUB)
            pre = fdot(x_ref[rows, :], w_ref[:, cols], NN)
            cdf = 0.5 + 0.5 * jnp.tanh(pre * (GELU_LIN + GELU_CUB * (pre * pre)))
            act_ref[rows, cols] = (pre * cdf).astype(jnp.bfloat16)


def forward_up(hidden, weight):
    tokens, width = hidden.shape
    ff = weight.shape[1]
    return pl.pallas_call(
        up_kernel,
        out_shape=jax.ShapeDtypeStruct((tokens, ff), jnp.bfloat16),
        grid=(tokens // TOK, ff // FF),
        in_specs=[pl.BlockSpec((TOK, width), lambda i, j: (i, 0)), pl.BlockSpec((width, FF), lambda i, j: (0, j))],
        out_specs=pl.BlockSpec((TOK, FF), lambda i, j: (i, j)),
        compiler_params=params(),
        cost_estimate=cost(2 * tokens * width * ff, 2 * tokens * width + 2 * tokens * ff + 2 * width * ff, tokens * ff),
        name="forward_up",
    )(hidden, weight)


def down_kernel(act_ref, w_ref, hidden_ref, *refs):
    out_ref, total = refs[-2:]
    k = pl.program_id(2)
    last = pl.num_programs(2) - 1

    @pl.when(k == 0)
    def _():
        total[...] = fdot(act_ref[...], w_ref[...], NN)

    @pl.when(jnp.logical_and(k > 0, k < last))
    def _():
        total[...] += fdot(act_ref[...], w_ref[...], NN)

    @pl.when(k == last)
    def _():
        out_ref[...] = (hidden_ref[...].astype(jnp.float32) + (total[...] + fdot(act_ref[...], w_ref[...], NN))).astype(jnp.bfloat16)


def forward_down(act, weight, hidden, col=0, earlier=()):
    tokens, ff = act.shape
    width = weight.shape[1]
    depth = DEPTH * WIDE // width
    tile = pl.BlockSpec((WIDE, width), lambda i, j, k: (i, col))
    return pl.pallas_call(
        down_kernel,
        out_shape=jax.ShapeDtypeStruct(hidden.shape, jnp.bfloat16),
        grid=(tokens // WIDE, 1, ff // depth),
        in_specs=[pl.BlockSpec((WIDE, depth), lambda i, j, k: (i, k)), pl.BlockSpec((depth, width), lambda i, j, k: (k, 0)), tile] + [pl.BlockSpec(memory_space=pl.ANY)] * len(earlier),
        out_specs=tile,
        scratch_shapes=[pltpu.VMEM((WIDE, width), jnp.float32)],
        input_output_aliases={3 + i: i for i in range(len(earlier))},
        compiler_params=params(),
        cost_estimate=cost(2 * tokens * width * ff, 2 * tokens * ff + 4 * tokens * width + 2 * width * ff),
        name="forward_down",
    )(act, weight, hidden, *earlier)


def pair_swap(value):
    return lax.ppermute(value, "fsdp", PAIR_SWAP)


def after(value, *first):
    return lax.optimization_barrier((value,) + first)[0]


def gradient_rows(x_saved, grad_out, w_up, w_down, gacc_up, gacc_down):
    layers, width, ff = w_up.shape
    core = lax.rem(lax.axis_index("fsdp"), 2).reshape(1)
    x_own = x_saved.reshape(-1, width)
    grad_own = grad_out.reshape(-1, width)
    tokens = grad_own.shape[0]
    x_peer, grad_peer = pair_swap(x_own), pair_swap(grad_own)
    rows_up, rows_down = [None] * layers, [None] * layers
    recv_down = None
    squares = []
    for layer in range(layers - 1, -1, -1):
        act_own, dpre_own = act_and_dpre(core, x_own, grad_own, w_up, w_down, layer)
        peer_core = after(core, act_own) if recv_down is None else after(core, act_own, recv_down)
        act_peer, dpre_peer = act_and_dpre(peer_core, x_peer, grad_peer, w_up, w_down, layer)
        old_grads = (grad_own, grad_peer)
        if layer > 0:
            from_peer = pair_swap(grad_back(core, dpre_peer, w_up, layer))
            grad_own = grad_back(core, dpre_own, w_up, layer, (grad_own, from_peer))
            grad_peer = pair_swap(grad_own)
        ranges = [(0, width)] if layer > 0 else [(2 * width // 3, width // 3), (0, 2 * width // 3)]
        order, partial_sums = core, []
        for start, cols in ranges:
            row_tile = WIDE if cols > 512 else 2 * WIDE
            part = token_dot(order, act_own, old_grads[0], act_peer, old_grads[1], tokens, (row_tile, cols), 0, cols, start // cols)
            recv_down = lax.all_to_all(part, "fsdp", 0, 0, tiled=True, axis_index_groups=SAME_CORE)
            partial_sums.append((recv_down, start))
            order = after(core, part)
        if len(ranges) > 1:
            order = after(order, partial_sums[0][0])
        part_up = token_dot(order, x_own, dpre_own, x_peer, dpre_peer, tokens, (WIDE, WIDE), layer)
        recv_up = lax.all_to_all(part_up, "fsdp", 0, 0, tiled=True)
        earlier = ()
        for recv, start in partial_sums:
            grad, sq = summed_down(recv, gacc_down, layer, start, earlier)
            earlier = (grad,)
            squares.append(sq)
        rows_down[layer] = grad
        rows_up[layer], sq = summed_up(recv_up, gacc_up, layer)
        squares.append(sq)
    return rows_up, rows_down, squares


def solution(mesh):
    n_dev = mesh.shape["fsdp"]
    rows_spec = P(None, "fsdp")

    def local_step(x_saved, grad_out, x_next, w_up, w_down, gacc_up, gacc_down, master_up, master_down, mom1_up, mom1_down, mom2_up, mom2_down):
        layers, width, ff = w_up.shape
        clip_norm = 0.1 * math.sqrt(2 * layers * width * ff)
        rows_up, rows_down, squares = gradient_rows(x_saved, grad_out, w_up, w_down, gacc_up, gacc_down)
        part = sum(jnp.sum(sq.reshape(8, -1, 128), axis=1) for sq in squares)
        clip = clip_factor(part, n_dev, clip_norm)
        new_up, new_down = (), ()
        up_shards, down_shards = [], []
        for layer in range(layers):
            *new_up, shard = adamw(clip, rows_up[layer], master_up, mom1_up, mom2_up, layer, (96, FF), new_up)
            up_shards.append(shard)
            *new_down, shard = adamw(clip, rows_down[layer], master_down, mom1_down, mom2_down, layer, (48, width), new_down)
            down_shards.append(shard)
        hidden = x_next.reshape(-1, width)
        for layer in range(layers):
            act = forward_up(hidden, lax.all_gather(up_shards[layer], "fsdp", axis=0, tiled=True))
            parts = 1 if layer < layers - 1 else 2
            cols = width // parts
            new_hidden = ()
            for part in range(parts):
                weight = lax.all_gather(down_shards[layer][:, part * cols:(part + 1) * cols], "fsdp", axis=0, tiled=True)
                new_hidden = (forward_down(act, weight, hidden, part, new_hidden),)
            hidden = new_hidden[0]
        return (hidden.reshape(x_next.shape), new_up[0], new_down[0], new_up[1], new_down[1], new_up[2], new_down[2])

    return jax.shard_map(local_step, mesh=mesh, in_specs=(rows_spec, P("fsdp"), P("fsdp"), P(), P(), rows_spec, rows_spec, rows_spec, rows_spec, rows_spec, rows_spec, rows_spec, rows_spec), out_specs=(P("fsdp"), rows_spec, rows_spec, rows_spec, rows_spec, rows_spec, rows_spec), check_vma=False)
```

```python
import functools
import math
import jax
import jax.numpy as jnp
from jax import lax
from jax.experimental import pallas as pl
from jax.experimental.pallas import tpu as pltpu
from jax.sharding import PartitionSpec as P

LEARN_RATE = 0.001
BETA_ONE = 0.9
BETA_TWO = 0.95
ADAM_EPS = 1e-8
WEIGHT_DECAY = 0.1
ADAM_STEP = 3
MICRO_STEPS = 2

GELU_LIN = 0.7978845608028654
GELU_CUB = GELU_LIN * 0.044715
PAIR_SWAP = [(0, 1), (1, 0), (2, 3), (3, 2), (4, 5), (5, 4), (6, 7), (7, 6)]
SAME_CORE = [[0, 2, 4, 6], [1, 3, 5, 7]]
LANES = 256
TOK = 1024
SUB = 256
FF = 768
DEPTH = 768
WIDE = 1536
VMEM_BYTES = 56 * 2**20
NN = (((1,), (0,)), ((), ()))
NT = (((1,), (1,)), ((), ()))
TN = (((0,), (0,)), ((), ()))


def fdot(left, right, dims):
    return lax.dot_general(left, right, dims, preferred_element_type=jnp.float32)


def params():
    return pltpu.CompilerParams(vmem_limit_bytes=VMEM_BYTES)


def cost(flops, moved, trans=0):
    return pl.CostEstimate(flops=int(flops), bytes_accessed=int(moved), transcendentals=int(trans))


def act_dpre_kernel(core_ref, x_ref, g_ref, up_ref, down_ref, act_ref, dpre_ref):
    for start in range(0, up_ref.shape[1], LANES):
        cols = slice(start, start + LANES)
        for top in range(0, x_ref.shape[0], SUB):
            rows = slice(top, top + SUB)
            pre = fdot(x_ref[rows, :], up_ref[:, cols], NN)
            d_act = fdot(g_ref[rows, :], down_ref[cols, :], NT)
            square = pre * pre
            cdf = 0.5 + 0.5 * jnp.tanh(pre * (GELU_LIN + GELU_CUB * square))
            act = pre * cdf
            slope = cdf + (act * (1.0 - cdf)) * (2.0 * GELU_LIN + 6.0 * GELU_CUB * square)
            act_ref[rows, cols] = act.astype(jnp.bfloat16)
            dpre_ref[rows, cols] = (d_act * slope).astype(jnp.bfloat16)


def act_and_dpre(core, x_all, grad, w_up, w_down, layer):
    tokens, width = grad.shape
    ff = w_up.shape[2]
    tiles = tokens // TOK
    spec = pltpu.PrefetchScalarGridSpec(
        num_scalar_prefetch=1,
        grid=(tiles, ff // FF // 2),
        in_specs=[
            pl.BlockSpec((TOK, width), lambda i, j, c: (layer * tiles + i, 0)),
            pl.BlockSpec((TOK, width), lambda i, j, c: (i, 0)),
            pl.BlockSpec((None, width, FF), lambda i, j, c: (layer, 0, 2 * j + c[0])),
            pl.BlockSpec((None, FF, width), lambda i, j, c: (layer, 2 * j + c[0], 0)),
        ],
        out_specs=[pl.BlockSpec((TOK, FF), lambda i, j, c: (i, j))] * 2,
    )
    return pl.pallas_call(
        act_dpre_kernel,
        out_shape=[jax.ShapeDtypeStruct((tokens, ff // 2), jnp.bfloat16)] * 2,
        grid_spec=spec,
        compiler_params=params(),
        cost_estimate=cost(2 * tokens * width * ff, 4 * tokens * width + 2 * tokens * ff + 6 * width * ff, tokens * ff // 2),
        name="act_dpre",
    )(core, x_all, grad, w_up, w_down)


def back_kernel(parts, final, core_ref, dpre_ref, *refs):
    w_refs, refs = refs[:parts], refs[parts:]
    out_ref = refs[-1]
    for start in range(0, out_ref.shape[1], LANES):
        cols = slice(start, start + LANES)
        total = fdot(dpre_ref[:, 0:FF], w_refs[0][cols, :], NT)
        for q in range(1, parts):
            total += fdot(dpre_ref[:, q * FF:(q + 1) * FF], w_refs[q][cols, :], NT)
        if final:
            total = refs[0][:, cols].astype(jnp.float32) + (total + refs[1][:, cols])
        out_ref[:, cols] = total.astype(out_ref.dtype)


def grad_back(core, dpre, w_up, layer, extra=()):
    tokens, half = dpre.shape
    width = w_up.shape[1]
    parts = half // FF
    col_tile = width // 2
    tile = pl.BlockSpec((TOK, col_tile), lambda i, j, c: (i, j))
    w_specs = [pl.BlockSpec((None, col_tile, FF), functools.partial(lambda q, i, j, c: (layer, j, 2 * q + c[0]), q)) for q in range(parts)]
    spec = pltpu.PrefetchScalarGridSpec(
        num_scalar_prefetch=1,
        grid=(tokens // TOK, width // col_tile),
        in_specs=[pl.BlockSpec((TOK, half), lambda i, j, c: (i, 0))] + w_specs + [tile] * len(extra),
        out_specs=tile,
    )
    return pl.pallas_call(
        functools.partial(back_kernel, parts, bool(extra)),
        out_shape=jax.ShapeDtypeStruct((tokens, width), jnp.bfloat16 if extra else jnp.float32),
        grid_spec=spec,
        compiler_params=params(),
        cost_estimate=cost(2 * tokens * half * width, 2 * tokens * half + 4 * width * half + 6 * tokens * width),
        name="grad_back",
    )(core, dpre, *([w_up] * parts), *extra)


def token_dot_kernel(order_ref, left_own, right_own, left_peer, right_peer, out_ref, total):
    k = pl.program_id(2)
    last = pl.num_programs(2) - 1
    odd = lax.rem(k, 2)

    @pl.when(k == 0)
    def _():
        total[...] = fdot(left_own[...], right_own[...], TN)

    @pl.when(jnp.logical_and(k > 0, odd == 0))
    def _():
        total[...] += fdot(left_own[...], right_own[...], TN)

    @pl.when(jnp.logical_and(k < last, odd == 1))
    def _():
        total[...] += fdot(left_peer[...], right_peer[...], TN)

    @pl.when(k == last)
    def _():
        out_ref[...] = (total[...] + fdot(left_peer[...], right_peer[...], TN)).astype(jnp.bfloat16)


def token_dot(order, left_own, right_own, left_peer, right_peer, tokens, tile, left_row=0, cols=None, right_col=0):
    rows = left_own.shape[1]
    cols = cols or right_own.shape[1]
    row_tile, col_tile = tile
    steps = tokens // DEPTH

    def left(own):
        return pl.BlockSpec((DEPTH, row_tile), lambda i, j, k, c: (left_row * steps + (k // 2 if own else jnp.maximum(k - 1, 0) // 2), i))

    def right(own):
        return pl.BlockSpec((DEPTH, col_tile), lambda i, j, k, c: (k // 2 if own else jnp.maximum(k - 1, 0) // 2, right_col + j))

    spec = pltpu.PrefetchScalarGridSpec(
        num_scalar_prefetch=1,
        grid=(rows // row_tile, cols // col_tile, 2 * steps),
        in_specs=[left(True), right(True), left(False), right(False)],
        out_specs=pl.BlockSpec((row_tile, col_tile), lambda i, j, k, c: (i, j)),
        scratch_shapes=[pltpu.VMEM((row_tile, col_tile), jnp.float32)],
    )
    return pl.pallas_call(
        token_dot_kernel,
        out_shape=jax.ShapeDtypeStruct((rows, cols), jnp.bfloat16),
        grid_spec=spec,
        compiler_params=params(),
        cost_estimate=cost(4 * tokens * rows * cols, 4 * tokens * (rows + cols) + 2 * rows * cols),
        name="token_dot",
    )(order, left_own, right_own, left_peer, right_peer)


def sum_kernel(halves, recv_ref, acc_ref, *refs):
    grad_ref, sq_ref = refs[-2:]
    cols = acc_ref.shape[1] // halves
    square = jnp.zeros((8, cols), jnp.float32)
    for half in range(halves):
        total = (recv_ref[0, half] if halves > 1 else recv_ref[0]).astype(jnp.float32)
        for src in range(1, recv_ref.shape[0]):
            total += (recv_ref[src, half] if halves > 1 else recv_ref[src]).astype(jnp.float32)
        part = slice(half * cols, (half + 1) * cols)
        grad = (acc_ref[:, part] + total) * (1.0 / MICRO_STEPS)
        grad_ref[:, part] = grad
        square += jnp.sum((grad * grad).reshape(-1, 8, cols), axis=0)
    first = jnp.logical_and(pl.program_id(0) == 0, pl.program_id(1) == 0)

    @pl.when(first)
    def _():
        sq_ref[...] = square

    @pl.when(jnp.logical_not(first))
    def _():
        sq_ref[...] += square


def summed(recv, gacc, layer, grid, recv_block, recv_index, tile, index, earlier=(), halves=1):
    rows, cols = gacc.shape[1:]
    moved = recv.size * 2 + recv.size * 2
    return pl.pallas_call(
        functools.partial(sum_kernel, halves),
        out_shape=[jax.ShapeDtypeStruct((rows, cols), jnp.float32), jax.ShapeDtypeStruct((8, tile[1] // halves), jnp.float32)],
        grid=grid,
        in_specs=[pl.BlockSpec(recv_block, recv_index), pl.BlockSpec((None,) + tile, lambda a, b: (layer,) + index(a, b))] + [pl.BlockSpec(memory_space=pl.ANY)] * len(earlier),
        out_specs=[pl.BlockSpec(tile, index), pl.BlockSpec((8, tile[1] // halves), lambda a, b: (0, 0))],
        input_output_aliases={2 + i: i for i in range(len(earlier))},
        compiler_params=params(),
        cost_estimate=cost(2 * recv.size, moved),
        name="grad_sum",
    )(recv, gacc, *earlier)


def summed_down(recv, gacc, layer, first_col, earlier=()):
    width = recv.shape[1]
    tile = (192, 512)
    skip = first_col // tile[1]
    return summed(recv.reshape(4, -1, width), gacc, layer, (4, width // tile[1]), (4,) + tile, lambda a, b: (0, a, b), tile, lambda a, b: (a, skip + b), earlier)


def summed_up(recv, gacc, layer):
    tile = (192, 2 * FF)
    return summed(recv.reshape(4, 2, -1, recv.shape[1]), gacc, layer, (4, 1), (4, 2, 192, FF), lambda a, b: (0, 0, 0, a), tile, lambda a, b: (0, a), (), 2)


def norm_kernel(n_dev, clip_norm, part_ref, clip_ref, slots, send_sem, recv_sem):
    me = lax.axis_index("fsdp")
    barrier = pltpu.get_barrier_semaphore()
    for step in range(1, n_dev):
        pl.semaphore_signal(barrier, inc=1, device_id=(lax.rem(me + step, n_dev),), device_id_type=pl.DeviceIdType.MESH)
    pl.semaphore_wait(barrier, n_dev - 1)

    def copy_to(step):
        return pltpu.make_async_remote_copy(
            src_ref=part_ref,
            dst_ref=slots.at[step],
            send_sem=send_sem.at[step],
            recv_sem=recv_sem.at[step],
            device_id=(lax.rem(me + step, n_dev),),
            device_id_type=pl.DeviceIdType.MESH,
        )

    for step in range(1, n_dev):
        copy_to(step).start()
    for step in range(1, n_dev):
        copy_to(step).wait()
    total = part_ref[...]
    for step in range(1, n_dev):
        total = total + slots[step]
    norm = jnp.sqrt(jnp.sum(total, keepdims=True))
    clip_ref[...] = jnp.broadcast_to(jnp.minimum(1.0, clip_norm / norm), clip_ref.shape)


def clip_factor(part, n_dev, clip_norm):
    return pl.pallas_call(
        functools.partial(norm_kernel, n_dev, clip_norm),
        out_shape=jax.ShapeDtypeStruct((8, 128), jnp.float32),
        in_specs=[pl.BlockSpec(memory_space=pltpu.VMEM)],
        out_specs=pl.BlockSpec(memory_space=pltpu.VMEM),
        scratch_shapes=[pltpu.VMEM((n_dev, 8, 128), jnp.float32), pltpu.SemaphoreType.DMA((n_dev,)), pltpu.SemaphoreType.DMA((n_dev,))],
        compiler_params=pltpu.CompilerParams(collective_id=0, has_side_effects=True),
        name="clip_norm",
    )(part)


def adamw_values(clip_ref, grad_ref, master_ref, one_ref, two_ref):
    grad = grad_ref[...] * clip_ref[0:1, 0:1]
    master = master_ref[...]
    one = BETA_ONE * one_ref[...] + (1.0 - BETA_ONE) * grad
    two = BETA_TWO * two_ref[...] + (1.0 - BETA_TWO) * grad * grad
    first_hat = one / (1.0 - BETA_ONE ** ADAM_STEP)
    second_hat = two / (1.0 - BETA_TWO ** ADAM_STEP)
    master = master - LEARN_RATE * (first_hat / (jnp.sqrt(second_hat) + ADAM_EPS) + WEIGHT_DECAY * master)
    return master, one, two


def adamw_kernel(aliased, weight, state, *refs):
    outs = list(refs[5 + aliased:])
    master, one, two = adamw_values(*refs[:5])
    if state:
        for value in (master, one, two):
            outs.pop(0)[...] = value
    if weight:
        outs.pop(0)[...] = master.astype(jnp.bfloat16)


def adamw(clip, grad, master, mom_one, mom_two, layer, tile, earlier=(), weight=True, state=True):
    rows, cols = grad.shape
    whole = pl.BlockSpec((None,) + tile, lambda a, b: (layer, a, b))
    part = pl.BlockSpec(tile, lambda a, b: (a, b))
    full = jax.ShapeDtypeStruct(master.shape, jnp.float32)
    return pl.pallas_call(
        functools.partial(adamw_kernel, len(earlier), weight, state),
        out_shape=[full] * (3 * state) + [jax.ShapeDtypeStruct((rows, cols), jnp.bfloat16)] * weight,
        grid=(rows // tile[0], cols // tile[1]),
        in_specs=[pl.BlockSpec((8, 128), lambda a, b: (0, 0)), part, whole, whole, whole] + [pl.BlockSpec(memory_space=pl.ANY)] * len(earlier),
        out_specs=[whole] * (3 * state) + [part] * weight,
        input_output_aliases={5 + i: i for i in range(len(earlier))},
        compiler_params=params(),
        cost_estimate=cost(20 * rows * cols, 16 * rows * cols + 12 * rows * cols * state, 2 * rows * cols),
        name="adamw",
    )(clip, grad, master, mom_one, mom_two, *earlier)


def up_kernel(x_ref, w_ref, act_ref):
    for start in range(0, w_ref.shape[1], LANES):
        cols = slice(start, start + LANES)
        for top in range(0, x_ref.shape[0], SUB):
            rows = slice(top, top + SUB)
            pre = fdot(x_ref[rows, :], w_ref[:, cols], NN)
            cdf = 0.5 + 0.5 * jnp.tanh(pre * (GELU_LIN + GELU_CUB * (pre * pre)))
            act_ref[rows, cols] = (pre * cdf).astype(jnp.bfloat16)


def forward_up(hidden, weight):
    tokens, width = hidden.shape
    ff = weight.shape[1]
    return pl.pallas_call(
        up_kernel,
        out_shape=jax.ShapeDtypeStruct((tokens, ff), jnp.bfloat16),
        grid=(tokens // TOK, ff // FF),
        in_specs=[pl.BlockSpec((TOK, width), lambda i, j: (i, 0)), pl.BlockSpec((width, FF), lambda i, j: (0, j))],
        out_specs=pl.BlockSpec((TOK, FF), lambda i, j: (i, j)),
        compiler_params=params(),
        cost_estimate=cost(2 * tokens * width * ff, 2 * tokens * width + 2 * tokens * ff + 2 * width * ff, tokens * ff),
        name="forward_up",
    )(hidden, weight)


def down_kernel(act_ref, w_ref, hidden_ref, *refs):
    out_ref, total = refs[-2:]
    k = pl.program_id(2)
    last = pl.num_programs(2) - 1

    @pl.when(k == 0)
    def _():
        total[...] = fdot(act_ref[...], w_ref[...], NN)

    @pl.when(jnp.logical_and(k > 0, k < last))
    def _():
        total[...] += fdot(act_ref[...], w_ref[...], NN)

    @pl.when(k == last)
    def _():
        out_ref[...] = (hidden_ref[...].astype(jnp.float32) + (total[...] + fdot(act_ref[...], w_ref[...], NN))).astype(jnp.bfloat16)


def forward_down(act, weight, hidden, col=0, earlier=()):
    tokens, ff = act.shape
    width = weight.shape[1]
    depth = DEPTH * WIDE // width
    tile = pl.BlockSpec((WIDE, width), lambda i, j, k: (i, col))
    return pl.pallas_call(
        down_kernel,
        out_shape=jax.ShapeDtypeStruct(hidden.shape, jnp.bfloat16),
        grid=(tokens // WIDE, 1, ff // depth),
        in_specs=[pl.BlockSpec((WIDE, depth), lambda i, j, k: (i, k)), pl.BlockSpec((depth, width), lambda i, j, k: (k, 0)), tile] + [pl.BlockSpec(memory_space=pl.ANY)] * len(earlier),
        out_specs=tile,
        scratch_shapes=[pltpu.VMEM((WIDE, width), jnp.float32)],
        input_output_aliases={3 + i: i for i in range(len(earlier))},
        compiler_params=params(),
        cost_estimate=cost(2 * tokens * width * ff, 2 * tokens * ff + 4 * tokens * width + 2 * width * ff),
        name="forward_down",
    )(act, weight, hidden, *earlier)


def pair_swap(value):
    return lax.ppermute(value, "fsdp", PAIR_SWAP)


def after(value, *first):
    return lax.optimization_barrier((value,) + first)[0]


def gradient_rows(x_saved, grad_out, w_up, w_down, gacc_up, gacc_down):
    layers, width, ff = w_up.shape
    core = lax.rem(lax.axis_index("fsdp"), 2).reshape(1)
    x_own = x_saved.reshape(-1, width)
    grad_own = grad_out.reshape(-1, width)
    tokens = grad_own.shape[0]
    x_peer, grad_peer = pair_swap(x_own), pair_swap(grad_own)
    rows_up, rows_down = [None] * layers, [None] * layers
    recv_down = None
    squares = []
    for layer in range(layers - 1, -1, -1):
        act_own, dpre_own = act_and_dpre(core, x_own, grad_own, w_up, w_down, layer)
        peer_core = after(core, act_own) if recv_down is None else after(core, act_own, recv_down)
        act_peer, dpre_peer = act_and_dpre(peer_core, x_peer, grad_peer, w_up, w_down, layer)
        old_grads = (grad_own, grad_peer)
        if layer > 0:
            from_peer = pair_swap(grad_back(core, dpre_peer, w_up, layer))
            grad_own = grad_back(core, dpre_own, w_up, layer, (grad_own, from_peer))
            grad_peer = pair_swap(grad_own)
        ranges = [(0, width)] if layer > 0 else [(2 * width // 3, width // 3), (0, 2 * width // 3)]
        order, partial_sums = core, []
        for start, cols in ranges:
            row_tile = WIDE if cols > 512 else 2 * WIDE
            part = token_dot(order, act_own, old_grads[0], act_peer, old_grads[1], tokens, (row_tile, cols), 0, cols, start // cols)
            recv_down = lax.all_to_all(part, "fsdp", 0, 0, tiled=True, axis_index_groups=SAME_CORE)
            partial_sums.append((recv_down, start))
            order = after(core, part)
        if len(ranges) > 1:
            order = after(order, partial_sums[0][0])
        part_up = token_dot(order, x_own, dpre_own, x_peer, dpre_peer, tokens, (WIDE, WIDE), layer)
        recv_up = lax.all_to_all(part_up, "fsdp", 0, 0, tiled=True)
        earlier = ()
        for recv, start in partial_sums:
            grad, sq = summed_down(recv, gacc_down, layer, start, earlier)
            earlier = (grad,)
            squares.append(sq)
        rows_down[layer] = grad
        rows_up[layer], sq = summed_up(recv_up, gacc_up, layer)
        squares.append(sq)
    return rows_up, rows_down, squares


def solution(mesh):
    n_dev = mesh.shape["fsdp"]
    rows_spec = P(None, "fsdp")

    def local_step(x_saved, grad_out, x_next, w_up, w_down, gacc_up, gacc_down, master_up, master_down, mom1_up, mom1_down, mom2_up, mom2_down):
        layers, width, ff = w_up.shape
        clip_norm = 0.1 * math.sqrt(2 * layers * width * ff)
        rows_up, rows_down, squares = gradient_rows(x_saved, grad_out, w_up, w_down, gacc_up, gacc_down)
        part = sum(jnp.sum(sq.reshape(8, -1, 128), axis=1) for sq in squares)
        clip = clip_factor(part, n_dev, clip_norm)
        new_up, new_down = (), ()
        up_shards, down_shards = [], []
        first_shard, = adamw(clip, rows_up[0], master_up, mom1_up, mom2_up, 0, (192, FF), (), True, False)
        later = after(clip, first_shard)
        for layer in range(layers):
            if layer == 0:
                new_up, shard = adamw(later, rows_up[0], master_up, mom1_up, mom2_up, 0, (192, FF), (), False, True), first_shard
            else:
                *new_up, shard = adamw(later, rows_up[layer], master_up, mom1_up, mom2_up, layer, (192, FF), new_up)
            up_shards.append(shard)
            *new_down, shard = adamw(later, rows_down[layer], master_down, mom1_down, mom2_down, layer, (96, width), new_down)
            down_shards.append(shard)
        hidden = x_next.reshape(-1, width)
        for layer in range(layers):
            act = forward_up(hidden, lax.all_gather(up_shards[layer], "fsdp", axis=0, tiled=True))
            parts = 1 if layer < layers - 1 else 2
            cols = width // parts
            new_hidden = ()
            for part in range(parts):
                weight = lax.all_gather(down_shards[layer][:, part * cols:(part + 1) * cols], "fsdp", axis=0, tiled=True)
                new_hidden = (forward_down(act, weight, hidden, part, new_hidden),)
            hidden = new_hidden[0]
        return (hidden.reshape(x_next.shape), new_up[0], new_down[0], new_up[1], new_down[1], new_up[2], new_down[2])

    return jax.shard_map(local_step, mesh=mesh, in_specs=(rows_spec, P("fsdp"), P("fsdp"), P(), P(), rows_spec, rows_spec, rows_spec, rows_spec, rows_spec, rows_spec, rows_spec, rows_spec), out_specs=(P("fsdp"), rows_spec, rows_spec, rows_spec, rows_spec, rows_spec, rows_spec), check_vma=False)
```
